32 devices in a mesh: seg: 8 (over z, y), bins: 4 (over x, core).
Axes of the slice: x: 2, y: 2, z: 4, core: 2. Of those that a mesh axis runs over, the one named last changes fastest.
Arguments:
- segment_maps: float32 [8, 32, 65536], P('seg', None, 'bins'), may hold values from 0 to 8
- bin_shifts: int32 [8, 32], P('seg'), may hold values from -64 to 64, as said below
- window_start: int32 [256], replicated, may hold values from 0 to 7
- window_length: int32 [256], replicated, may hold values from 1 to 8, as said below
Outputs:
- peak_score: float32 [32, 65536], P(None, ('bins', 'seg'))
The draws below stay inside these ranges and needn't reach their ends.
Inputs may be any that keep to these rules, and one draw needn't show every extreme that they name: `bin_shifts`: both 64 and -64 occur in every draw. window_start + window_length <= 8 for every window; every draw has a window of all 8 segments and a window of one segment.
All inputs are finite; a program needn't handle non-finite values.
Results may differ from the reference program's by a relative error of at most 0.0003.
Values sent between devices are 32-bit elements; how exact they have to be, the bound alone decides.
A program may use at most 256 MiB of HBM per device.

```python
import jax
import jax.numpy as jnp
from jax import lax

SPIN = 32
HALO = 64
NWIN = 256
NSEG = 8
FREQS = 65536


def window_tables(key):
    key = jax.random.fold_in(key, 7071)
    first_key, second_key, third_key = jax.random.split(key, 3)
    opening = jax.random.randint(first_key, (NWIN,), 0, NSEG)
    extra = jax.random.randint(second_key, (NWIN,), 0, 1 << 20)
    length = 1 + extra % (NSEG - opening)
    chosen = jax.random.randint(third_key, (), 0, NWIN)
    partner = (chosen + NWIN // 2) % NWIN
    positions = jnp.arange(NWIN)
    opening = jnp.where(positions == chosen, 0, jnp.where(positions == partner, NSEG - 1, opening))
    length = jnp.where(positions == chosen, NSEG, jnp.where(positions == partner, 1, length))
    return (opening.astype(jnp.int32), length.astype(jnp.int32))


def draw_window_start(key, part):
    return window_tables(key)[0]


def draw_window_length(key, part):
    return window_tables(key)[1]


def draw_bin_shifts(key, part):
    key = jax.random.fold_in(key, 313)
    first_key, second_key, third_key = jax.random.split(key, 3)
    values = jax.random.randint(first_key, (NSEG, SPIN), -HALO, HALO + 1)
    flat = jnp.arange(NSEG * SPIN).reshape(NSEG, SPIN)
    upward = jax.random.randint(second_key, (), 0, NSEG * SPIN)
    downward = (upward + 1 + jax.random.randint(third_key, (), 0, NSEG * SPIN - 1)) % (NSEG * SPIN)
    values = jnp.where(flat == upward, HALO, jnp.where(flat == downward, -HALO, values))
    return values.astype(jnp.int32)


def levels(own_key, shape, cuts, smallest, largest):
    factor_of, own = 1.0, jax.random.fold_in(own_key, 6)
    for dim, blocks in cuts:
        heights = jnp.exp(jax.random.uniform(jax.random.fold_in(own, dim), (blocks,), jnp.float32, smallest / len(cuts), largest / len(cuts)))
        factor_of = factor_of * jnp.repeat(heights, shape[dim] // blocks).reshape([-1 if axis == dim else 1 for axis in range(len(shape))])
    return factor_of


def setup_inputs(seed: int = 0) -> dict:
    key_of = jax.random.split(jax.random.key(seed), 5)
    segment_maps = jnp.clip(8.0 * jax.random.uniform(key_of[0], (NSEG, SPIN, FREQS), jnp.float32) ** levels(key_of[0], (NSEG, SPIN, FREQS), ((0, 8), (2, 4)), -0.2, 0.2), 0.0, 8.0)
    bin_shifts = draw_bin_shifts(jax.random.fold_in(key_of[4], 71), 0)
    window_start = draw_window_start(jax.random.fold_in(key_of[4], 71), 0)
    window_length = draw_window_length(jax.random.fold_in(key_of[4], 71), 0)
    return {"segment_maps": segment_maps, "bin_shifts": bin_shifts, "window_start": window_start, "window_length": window_length}


def align_spin(spin_index, segment_maps, bin_shifts):
    column = lax.dynamic_index_in_dim(segment_maps, spin_index, 1, keepdims=False)
    offsets = lax.dynamic_index_in_dim(bin_shifts, spin_index, 1, keepdims=False)
    padded = jnp.pad(column, ((0, 0), (HALO, HALO)))

    def extract(values, amount):
        return lax.dynamic_slice_in_dim(values, (amount + HALO).astype(jnp.int32), FREQS)
    return jax.vmap(extract)(padded, offsets)

def reference(segment_maps, bin_shifts, window_start, window_length):
    finish = (window_start + window_length).astype(jnp.int32)
    opening = window_start.astype(jnp.int32)
    weight = window_length.astype(jnp.float32)[:, None]

    def per_spin(spin_index):
        aligned = align_spin(spin_index, segment_maps, bin_shifts)
        cumulative = jnp.cumsum(aligned, axis=0)
        prefix = jnp.concatenate([jnp.zeros((1, FREQS), jnp.float32), cumulative], axis=0)
        totals = jnp.take(prefix, finish, axis=0) - jnp.take(prefix, opening, axis=0)
        scores = (totals - 4.0 * weight) / jnp.sqrt(8.0 * weight)
        return lax.optimization_barrier(jnp.max(scores, axis=0))
    return lax.map(per_spin, jnp.arange(SPIN, dtype=jnp.int32))
```

```python
import functools
import math

import jax
import jax.numpy as jnp
from jax import lax
from jax.experimental import pallas as pl
from jax.experimental.pallas import tpu as pltpu
from jax.sharding import PartitionSpec as P

MESH = pl.DeviceIdType.MESH
LANES = 128
ROWS = 8


def nearest(me, rank, n):
    short = jnp.minimum(me, n - 1 - me)
    up = me < n - 1 - me
    half = (rank + 1) // 2
    both = jnp.where(rank % 2 == 1, half, -half)
    rest = jnp.where(up, rank - short, short - rank)
    return me + jnp.where(rank <= 2 * short, both, rest)


def kernel(n, bands, by_pairs, maps, shifts, starts, lengths, out, wide, blocks, shift_rows, table,
           in_sem, send_sem, recv_sem, halo_send, halo_recv):
    me, band = lax.axis_index("seg"), lax.axis_index("bins")
    spins, bins = maps.shape[1], maps.shape[2]
    width = out.shape[1]
    tiles = width // LANES
    chunks = spins // ROWS
    windows = starts.shape[0]

    def rows_of(chunk):
        return pl.ds(pl.multiple_of(chunk * ROWS, ROWS), ROWS)

    def loading(chunk):
        return pltpu.make_async_copy(
            maps.at[0, rows_of(chunk), :], wide.at[rows_of(chunk), pl.ds(LANES, bins)], in_sem.at[chunk]
        )

    for chunk in range(chunks):
        loading(chunk).start()

    barrier = pltpu.get_barrier_semaphore()

    def greet(offset, carry):
        peer = lax.rem(me + offset, n)
        pl.semaphore_signal(barrier, inc=1, device_id={"seg": peer}, device_id_type=MESH)
        return carry

    lax.fori_loop(1, n, greet, 0)

    @pl.when(band > 0)
    def _():
        pl.semaphore_signal(barrier, inc=1, device_id={"bins": band - 1}, device_id_type=MESH)

    @pl.when(band < bands - 1)
    def _():
        pl.semaphore_signal(barrier, inc=1, device_id={"bins": band + 1}, device_id_type=MESH)

    @pl.when(band == 0)
    def _():
        wide[:, :LANES] = jnp.zeros((spins, LANES), jnp.float32)

    @pl.when(band == bands - 1)
    def _():
        wide[:, bins + LANES:] = jnp.zeros((spins, LANES), jnp.float32)

    sublane = lax.broadcasted_iota(jnp.int32, (ROWS, LANES), 0)
    lane = lax.broadcasted_iota(jnp.int32, (ROWS, LANES), 1)
    for chunk in range(chunks):
        amounts = jnp.zeros((ROWS, LANES), jnp.int32)
        for row in range(ROWS):
            amounts = jnp.where(sublane == row, shifts[0, chunk * ROWS + row], amounts)
        shift_rows[chunk * ROWS:(chunk + 1) * ROWS, :] = amounts

    neighbours = jnp.where(band > 0, 1, 0) + jnp.where(band < bands - 1, 1, 0)
    pl.semaphore_wait(barrier, n - 1 + neighbours)

    def halo(side, peer):
        source = bins - LANES if side == 0 else 0
        target = 0 if side == 0 else bins + LANES
        return pltpu.make_async_remote_copy(
            src_ref=maps.at[0, :, pl.ds(source, LANES)],
            dst_ref=wide.at[:, pl.ds(target, LANES)],
            send_sem=halo_send.at[side],
            recv_sem=halo_recv.at[side],
            device_id={"bins": peer},
            device_id_type=MESH,
        )

    @pl.when(band < bands - 1)
    def _():
        halo(0, band + 1).start()

    @pl.when(band > 0)
    def _():
        halo(1, band - 1).start()

    def sending(chunk, peer):
        return pltpu.make_async_remote_copy(
            src_ref=blocks.at[0, peer, rows_of(chunk), :],
            dst_ref=blocks.at[1, me, rows_of(chunk), :],
            send_sem=send_sem.at[chunk, peer],
            recv_sem=recv_sem.at[chunk, me],
            device_id={"seg": peer},
            device_id_type=MESH,
        )

    def receiving(chunk, source):
        return pltpu.make_async_remote_copy(
            src_ref=blocks.at[0, source, rows_of(chunk), :],
            dst_ref=blocks.at[1, source, rows_of(chunk), :],
            send_sem=send_sem.at[chunk, source],
            recv_sem=recv_sem.at[chunk, source],
            device_id={"seg": source},
            device_id_type=MESH,
        )

    def step(i, carry):
        chunk, place = i // n, i % n
        own = place == n - 1
        dest = jnp.where(own, me, nearest(me, place + 1, n))

        @pl.when(place == 0)
        def _():
            loading(chunk).wait()

        @pl.when((chunk == 0) & (dest == 0) & (band > 0))
        def _():
            halo(0, band - 1).wait_recv()

        @pl.when((chunk == 0) & (dest == n - 1) & (band < bands - 1))
        def _():
            halo(1, band + 1).wait_recv()

        rows = rows_of(chunk)
        position = lane + shift_rows[rows, :]
        index = position & (LANES - 1)
        below, above = position < 0, position >= LANES

        def turned(tile):
            columns = pl.ds(pl.multiple_of(dest * width + tile * LANES, LANES), LANES)
            return jnp.take_along_axis(wide[rows, columns], index, axis=1, mode="promise_in_bounds")

        side = jnp.where(own, 1, 0)
        before, here = turned(0), turned(1)
        for tile in range(tiles):
            after = turned(tile + 2)
            blocks[side, dest, rows, tile * LANES:(tile + 1) * LANES] = jnp.where(
                below, before, jnp.where(above, after, here)
            )
            before, here = here, after

        @pl.when(place > 0)
        def _():
            sending(chunk, nearest(me, place, n)).start()

        return carry

    lax.fori_loop(0, chunks * n, step, 0)

    lowest = -jnp.inf
    if by_pairs:
        pair = lax.broadcasted_iota(jnp.int32, (n * n, LANES), 0)

        def mark(w, held):
            return jnp.where(pair == starts[w] * n + lengths[w] - 1, 0.0, held)

        table[...] = lax.fori_loop(0, windows, mark, jnp.full((n * n, LANES), lowest, jnp.float32))

    group = 2 * LANES if width % (2 * LANES) == 0 else LANES

    def arrive(chunk):
        def one(source, carry):
            @pl.when(source != me)
            def _():
                receiving(chunk, source).wait_recv()
            return carry
        lax.fori_loop(0, n, one, 0)

    def search_pairs(chunk):
        rows = rows_of(chunk)

        def search(j, carry):
            columns = pl.ds(pl.multiple_of(j * group, group), group)
            prefix = [None]
            for source in range(n):
                value = blocks[1, source, rows, columns]
                prefix.append(value if source == 0 else prefix[-1] + value)
            best = None
            for length in range(1, n + 1):
                most = None
                for start in range(n + 1 - length):
                    total = prefix[length] if start == 0 else prefix[start + length] - prefix[start]
                    at = start * n + length - 1
                    mask = jnp.concatenate([table[at:at + 1, :]] * (group // LANES), axis=1)
                    total = total + mask
                    most = total if most is None else jnp.maximum(most, total)
                root = math.sqrt(8.0 * length)
                score = most * (1.0 / root) - 4.0 * length / root
                best = score if best is None else jnp.maximum(best, score)
            out[rows, columns] = best
            return carry

        lax.fori_loop(0, width // group, search, 0)

    def search_windows(chunk):
        rows = rows_of(chunk)
        table[0] = jnp.zeros((ROWS, width), jnp.float32)

        def add(source, total):
            total = total + blocks[1, source, rows, :]
            table[source + 1] = total
            return total

        lax.fori_loop(0, n, add, jnp.zeros((ROWS, width), jnp.float32))

        def search(w, best):
            total = table[starts[w] + lengths[w]] - table[starts[w]]
            weight = jnp.full((ROWS, width), lengths[w], jnp.int32).astype(jnp.float32)
            return jnp.maximum(best, (total - 4.0 * weight) / jnp.sqrt(8.0 * weight))

        out[rows, :] = lax.fori_loop(0, windows, search, jnp.full((ROWS, width), lowest, jnp.float32))

    def finish(chunk, carry):
        arrive(chunk)
        (search_pairs if by_pairs else search_windows)(chunk)
        return carry

    lax.fori_loop(0, chunks, finish, 0)

    def drain(i, carry):
        chunk, peer = i // n, i % n

        @pl.when(peer != me)
        def _():
            sending(chunk, peer).wait_send()
        return carry

    lax.fori_loop(0, chunks * n, drain, 0)

    @pl.when(band < bands - 1)
    def _():
        halo(0, band + 1).wait_send()

    @pl.when(band > 0)
    def _():
        halo(1, band - 1).wait_send()


def solution(mesh):
    n, bands = mesh.shape["seg"], mesh.shape["bins"]

    def on_device(segment_maps, bin_shifts, window_start, window_length):
        _, spins, bins = segment_maps.shape
        width = bins // n
        chunks = spins // ROWS
        by_pairs = n * (n + 1) // 2 <= window_start.shape[0]
        table = (n * n, LANES) if by_pairs else (n + 1, ROWS, width)
        smem = pl.BlockSpec(memory_space=pltpu.SMEM)
        return pl.pallas_call(
            functools.partial(kernel, n, bands, by_pairs),
            out_shape=jax.ShapeDtypeStruct((spins, width), jnp.float32),
            in_specs=[pl.BlockSpec(memory_space=pl.ANY), smem, smem, smem],
            out_specs=pl.BlockSpec(memory_space=pltpu.VMEM),
            scratch_shapes=[
                pltpu.VMEM((spins, bins + 2 * LANES), jnp.float32),
                pltpu.VMEM((2, n, spins, width), jnp.float32),
                pltpu.VMEM((spins, LANES), jnp.int32),
                pltpu.VMEM(table, jnp.float32),
                pltpu.SemaphoreType.DMA((chunks,)),
                pltpu.SemaphoreType.DMA((chunks, n)),
                pltpu.SemaphoreType.DMA((chunks, n)),
                pltpu.SemaphoreType.DMA((2,)),
                pltpu.SemaphoreType.DMA((2,)),
            ],
            compiler_params=pltpu.CompilerParams(collective_id=0, has_side_effects=True),
        )(segment_maps, bin_shifts, window_start, window_length)

    return jax.shard_map(
        on_device,
        mesh=mesh,
        in_specs=(P("seg", None, "bins"), P("seg", None), P(), P()),
        out_specs=P(None, ("bins", "seg")),
        check_vma=False,
    )
```

```python
import functools
import math

import jax
import jax.numpy as jnp
from jax import lax
from jax.experimental import pallas as pl
from jax.experimental.pallas import tpu as pltpu
from jax.sharding import PartitionSpec as P

MESH = pl.DeviceIdType.MESH
LANES = 128
ROWS = 8


def order(me, place, n):
    stride = n // 2
    first, partner = 0, place + stride
    while stride > 1:
        first += stride
        stride //= 2
        partner = jnp.where(place >= first, place - first + stride, partner)
    other, bit = 0, 1
    while bit < n:
        other = other + (me // bit + partner // bit) % 2 * bit
        bit *= 2
    return other


def kernel(n, bands, by_pairs, maps, shifts, starts, lengths, out, wide, blocks, shift_rows, table,
           in_sem, send_sem, recv_sem, halo_send, halo_recv):
    me, band = lax.axis_index("seg"), lax.axis_index("bins")
    spins, bins = maps.shape[1], maps.shape[2]
    width = out.shape[1]
    tiles = width // LANES
    chunks = spins // ROWS
    windows = starts.shape[0]

    def rows_of(chunk):
        return pl.ds(pl.multiple_of(chunk * ROWS, ROWS), ROWS)

    def loading(chunk):
        return pltpu.make_async_copy(
            maps.at[0, rows_of(chunk), :], wide.at[rows_of(chunk), pl.ds(LANES, bins)], in_sem.at[chunk]
        )

    for chunk in range(chunks):
        loading(chunk).start()

    barrier = pltpu.get_barrier_semaphore()

    def greet(offset, carry):
        peer = lax.rem(me + offset, n)
        pl.semaphore_signal(barrier, inc=1, device_id={"seg": peer}, device_id_type=MESH)
        return carry

    lax.fori_loop(1, n, greet, 0)

    @pl.when(band > 0)
    def _():
        pl.semaphore_signal(barrier, inc=1, device_id={"bins": band - 1}, device_id_type=MESH)

    @pl.when(band < bands - 1)
    def _():
        pl.semaphore_signal(barrier, inc=1, device_id={"bins": band + 1}, device_id_type=MESH)

    @pl.when(band == 0)
    def _():
        wide[:, :LANES] = jnp.zeros((spins, LANES), jnp.float32)

    @pl.when(band == bands - 1)
    def _():
        wide[:, bins + LANES:] = jnp.zeros((spins, LANES), jnp.float32)

    sublane = lax.broadcasted_iota(jnp.int32, (ROWS, LANES), 0)
    lane = lax.broadcasted_iota(jnp.int32, (ROWS, LANES), 1)
    for chunk in range(chunks):
        amounts = jnp.zeros((ROWS, LANES), jnp.int32)
        for row in range(ROWS):
            amounts = jnp.where(sublane == row, shifts[0, chunk * ROWS + row], amounts)
        shift_rows[chunk * ROWS:(chunk + 1) * ROWS, :] = amounts

    neighbours = jnp.where(band > 0, 1, 0) + jnp.where(band < bands - 1, 1, 0)
    pl.semaphore_wait(barrier, n - 1 + neighbours)

    def halo(side, peer):
        source = bins - LANES if side == 0 else 0
        target = 0 if side == 0 else bins + LANES
        return pltpu.make_async_remote_copy(
            src_ref=maps.at[0, :, pl.ds(source, LANES)],
            dst_ref=wide.at[:, pl.ds(target, LANES)],
            send_sem=halo_send.at[side],
            recv_sem=halo_recv.at[side],
            device_id={"bins": peer},
            device_id_type=MESH,
        )

    @pl.when(band < bands - 1)
    def _():
        halo(0, band + 1).start()

    @pl.when(band > 0)
    def _():
        halo(1, band - 1).start()

    def sending(chunk, peer):
        return pltpu.make_async_remote_copy(
            src_ref=blocks.at[0, peer, rows_of(chunk), :],
            dst_ref=blocks.at[1, me, rows_of(chunk), :],
            send_sem=send_sem.at[chunk, peer],
            recv_sem=recv_sem.at[chunk, me],
            device_id={"seg": peer},
            device_id_type=MESH,
        )

    def receiving(chunk, source):
        return pltpu.make_async_remote_copy(
            src_ref=blocks.at[0, source, rows_of(chunk), :],
            dst_ref=blocks.at[1, source, rows_of(chunk), :],
            send_sem=send_sem.at[chunk, source],
            recv_sem=recv_sem.at[chunk, source],
            device_id={"seg": source},
            device_id_type=MESH,
        )

    def step(i, carry):
        chunk, place = i // n, i % n
        own = place == n - 1
        dest = jnp.where(own, me, order(me, place, n))

        @pl.when(place == 0)
        def _():
            loading(chunk).wait()

        @pl.when((chunk == 0) & (dest == 0) & (band > 0))
        def _():
            halo(0, band - 1).wait_recv()

        @pl.when((chunk == 0) & (dest == n - 1) & (band < bands - 1))
        def _():
            halo(1, band + 1).wait_recv()

        rows = rows_of(chunk)
        position = lane + shift_rows[rows, :]
        index = position & (LANES - 1)
        below, above = position < 0, position >= LANES

        def turned(tile):
            columns = pl.ds(pl.multiple_of(dest * width + tile * LANES, LANES), LANES)
            return jnp.take_along_axis(wide[rows, columns], index, axis=1, mode="promise_in_bounds")

        side = jnp.where(own, 1, 0)
        before, here = turned(0), turned(1)
        for tile in range(tiles):
            after = turned(tile + 2)
            blocks[side, dest, rows, tile * LANES:(tile + 1) * LANES] = jnp.where(
                below, before, jnp.where(above, after, here)
            )
            before, here = here, after

        @pl.when(place > 0)
        def _():
            sending(chunk, order(me, place - 1, n)).start()

        return carry

    lax.fori_loop(0, chunks * n, step, 0)

    lowest = -jnp.inf
    if by_pairs:
        pair = lax.broadcasted_iota(jnp.int32, (n * n, LANES), 0)

        def mark(w, held):
            return jnp.where(pair == starts[w] * n + lengths[w] - 1, 0.0, held)

        table[...] = lax.fori_loop(0, windows, mark, jnp.full((n * n, LANES), lowest, jnp.float32))

    group = 2 * LANES if width % (2 * LANES) == 0 else LANES

    def arrive(chunk):
        def one(source, carry):
            @pl.when(source != me)
            def _():
                receiving(chunk, source).wait_recv()
            return carry
        lax.fori_loop(0, n, one, 0)

    def search_pairs(chunk):
        rows = rows_of(chunk)

        def search(j, carry):
            columns = pl.ds(pl.multiple_of(j * group, group), group)
            prefix = [None]
            for source in range(n):
                value = blocks[1, source, rows, columns]
                prefix.append(value if source == 0 else prefix[-1] + value)
            best = None
            for length in range(1, n + 1):
                most = None
                for start in range(n + 1 - length):
                    total = prefix[length] if start == 0 else prefix[start + length] - prefix[start]
                    at = start * n + length - 1
                    mask = jnp.concatenate([table[at:at + 1, :]] * (group // LANES), axis=1)
                    total = total + mask
                    most = total if most is None else jnp.maximum(most, total)
                root = math.sqrt(8.0 * length)
                score = most * (1.0 / root) - 4.0 * length / root
                best = score if best is None else jnp.maximum(best, score)
            out[rows, columns] = best
            return carry

        lax.fori_loop(0, width // group, search, 0)

    def search_windows(chunk):
        rows = rows_of(chunk)
        table[0] = jnp.zeros((ROWS, width), jnp.float32)

        def add(source, total):
            total = total + blocks[1, source, rows, :]
            table[source + 1] = total
            return total

        lax.fori_loop(0, n, add, jnp.zeros((ROWS, width), jnp.float32))

        def search(w, best):
            total = table[starts[w] + lengths[w]] - table[starts[w]]
            weight = jnp.full((ROWS, width), lengths[w], jnp.int32).astype(jnp.float32)
            return jnp.maximum(best, (total - 4.0 * weight) / jnp.sqrt(8.0 * weight))

        out[rows, :] = lax.fori_loop(0, windows, search, jnp.full((ROWS, width), lowest, jnp.float32))

    def finish(chunk, carry):
        arrive(chunk)
        (search_pairs if by_pairs else search_windows)(chunk)
        return carry

    lax.fori_loop(0, chunks, finish, 0)

    def drain(i, carry):
        chunk, peer = i // n, i % n

        @pl.when(peer != me)
        def _():
            sending(chunk, peer).wait_send()
        return carry

    lax.fori_loop(0, chunks * n, drain, 0)

    @pl.when(band < bands - 1)
    def _():
        halo(0, band + 1).wait_send()

    @pl.when(band > 0)
    def _():
        halo(1, band - 1).wait_send()


def solution(mesh):
    n, bands = mesh.shape["seg"], mesh.shape["bins"]

    def on_device(segment_maps, bin_shifts, window_start, window_length):
        _, spins, bins = segment_maps.shape
        width = bins // n
        chunks = spins // ROWS
        by_pairs = n * (n + 1) // 2 <= window_start.shape[0]
        table = (n * n, LANES) if by_pairs else (n + 1, ROWS, width)
        smem = pl.BlockSpec(memory_space=pltpu.SMEM)
        return pl.pallas_call(
            functools.partial(kernel, n, bands, by_pairs),
            out_shape=pltpu.VMEM((spins, width), jnp.float32),
            in_specs=[pl.BlockSpec(memory_space=pl.ANY), smem, smem, smem],
            out_specs=pl.BlockSpec(memory_space=pltpu.VMEM),
            scratch_shapes=[
                pltpu.VMEM((spins, bins + 2 * LANES), jnp.float32),
                pltpu.VMEM((2, n, spins, width), jnp.float32),
                pltpu.VMEM((spins, LANES), jnp.int32),
                pltpu.VMEM(table, jnp.float32),
                pltpu.SemaphoreType.DMA((chunks,)),
                pltpu.SemaphoreType.DMA((chunks, n)),
                pltpu.SemaphoreType.DMA((chunks, n)),
                pltpu.SemaphoreType.DMA((2,)),
                pltpu.SemaphoreType.DMA((2,)),
            ],
            compiler_params=pltpu.CompilerParams(collective_id=0, has_side_effects=True),
        )(segment_maps, bin_shifts, window_start, window_length)

    return jax.shard_map(
        on_device,
        mesh=mesh,
        in_specs=(P("seg", None, "bins"), P("seg", None), P(), P()),
        out_specs=P(None, ("bins", "seg")),
        check_vma=False,
    )
```

```python
import functools
import math

import jax
import jax.numpy as jnp
from jax import lax
from jax.experimental import pallas as pl
from jax.experimental.pallas import tpu as pltpu
from jax.sharding import PartitionSpec as P

MESH = pl.DeviceIdType.MESH
LANES = 128
ROWS = 8


def order(me, place, n):
    stride = n // 2
    first, partner = 0, place + stride
    while stride > 1:
        first += stride
        stride //= 2
        partner = jnp.where(place >= first, place - first + stride, partner)
    return flipped(me, partner, n)


def flipped(me, mask, n):
    other, bit = 0, 1
    while bit < n:
        other = other + (me // bit + mask // bit) % 2 * bit
        bit *= 2
    return other


def twin(me):
    return me + 1 - 2 * (me % 2)


def kernel(n, bands, by_pairs, maps, shifts_in, starts_in, lengths_in, out, wide, blocks, shift_rows, table,
           shifts, starts, lengths, side_in, all_in, small_sem, in_sem, send_sem, recv_sem, halo_send, halo_recv):
    me, band = lax.axis_index("seg"), lax.axis_index("bins")
    spins, bins = maps.shape[1], maps.shape[2]
    width = out.shape[1]
    tiles = width // LANES
    chunks = spins // ROWS
    windows = starts.shape[0]

    def rows_of(chunk):
        return pl.ds(pl.multiple_of(chunk * ROWS, ROWS), ROWS)

    def loading(chunk):
        return pltpu.make_async_copy(
            maps.at[0, rows_of(chunk), :], wide.at[rows_of(chunk), pl.ds(LANES, bins)], in_sem.at[chunk]
        )

    barrier = pltpu.get_barrier_semaphore()

    def greet(peer):
        pl.semaphore_signal(barrier, inc=1, device_id={"seg": peer}, device_id_type=MESH)

    early = n // 2 == 4
    pairs, pair_at = n // 2, me // 2
    low = pair_at < pairs // 2
    inner, outer = jnp.where(low, me + 2, me - 2), jnp.where(low, me - 2, me + 2)
    middle = jnp.where(low, pair_at == pairs // 2 - 1, pair_at == pairs // 2)
    has_outer = jnp.where(low, pair_at > 0, pair_at < pairs - 1)

    greet(twin(me))

    @pl.when(middle)
    def _():
        greet(inner)
        greet(twin(inner))

    @pl.when(has_outer)
    def _():
        greet(outer)
        greet(twin(outer))

    @pl.when(band > 0)
    def _():
        pl.semaphore_signal(barrier, inc=1, device_id={"bins": band - 1}, device_id_type=MESH)

    @pl.when(band < bands - 1)
    def _():
        pl.semaphore_signal(barrier, inc=1, device_id={"bins": band + 1}, device_id_type=MESH)

    small = [
        pltpu.make_async_copy(here, there, small_sem.at[i])
        for i, (here, there) in enumerate(((shifts_in, shifts), (starts_in, starts), (lengths_in, lengths)))
    ]
    for copy in small:
        copy.start()
    for chunk in range(chunks):
        loading(chunk).start()

    @pl.when(band == 0)
    def _():
        wide[:, :LANES] = jnp.zeros((spins, LANES), jnp.float32)

    @pl.when(band == bands - 1)
    def _():
        wide[:, bins + LANES:] = jnp.zeros((spins, LANES), jnp.float32)

    for copy in small:
        copy.wait()

    sublane = lax.broadcasted_iota(jnp.int32, (ROWS, LANES), 0)
    lane = lax.broadcasted_iota(jnp.int32, (ROWS, LANES), 1)
    for chunk in range(chunks):
        amounts = jnp.zeros((ROWS, LANES), jnp.int32)
        for row in range(ROWS):
            amounts = jnp.where(sublane == row, shifts[0, chunk * ROWS + row], amounts)
        shift_rows[chunk * ROWS:(chunk + 1) * ROWS, :] = amounts

    neighbours = jnp.where(band > 0, 1, 0) + jnp.where(band < bands - 1, 1, 0)
    pl.semaphore_wait(barrier, 3 + neighbours)

    def tell(sem, peer):
        pl.semaphore_signal(sem, inc=1, device_id={"seg": peer}, device_id_type=MESH)

    @pl.when(jnp.logical_not(has_outer))
    def _():
        tell(side_in, inner)

    def hear_side():
        @pl.when(has_outer)
        def _():
            pl.semaphore_wait(side_in, 1)

        @pl.when(has_outer & middle)
        def _():
            tell(all_in, inner)

        @pl.when(has_outer & jnp.logical_not(middle))
        def _():
            tell(side_in, inner)

    def hear_all():
        pl.semaphore_wait(all_in, 1)

        @pl.when(has_outer)
        def _():
            tell(all_in, outer)

    if not early:
        hear_side()
        hear_all()

    def halo(side, peer):
        source = bins - LANES if side == 0 else 0
        target = 0 if side == 0 else bins + LANES
        return pltpu.make_async_remote_copy(
            src_ref=maps.at[0, :, pl.ds(source, LANES)],
            dst_ref=wide.at[:, pl.ds(target, LANES)],
            send_sem=halo_send.at[side],
            recv_sem=halo_recv.at[side],
            device_id={"bins": peer},
            device_id_type=MESH,
        )

    @pl.when(band < bands - 1)
    def _():
        halo(0, band + 1).start()

    @pl.when(band > 0)
    def _():
        halo(1, band - 1).start()

    def sending(chunk, peer):
        return pltpu.make_async_remote_copy(
            src_ref=blocks.at[0, peer, rows_of(chunk), :],
            dst_ref=blocks.at[1, me, rows_of(chunk), :],
            send_sem=send_sem.at[chunk, peer],
            recv_sem=recv_sem.at[chunk, me],
            device_id={"seg": peer},
            device_id_type=MESH,
        )

    def receiving(chunk, source):
        return pltpu.make_async_remote_copy(
            src_ref=blocks.at[0, source, rows_of(chunk), :],
            dst_ref=blocks.at[1, source, rows_of(chunk), :],
            send_sem=send_sem.at[chunk, source],
            recv_sem=recv_sem.at[chunk, source],
            device_id={"seg": source},
            device_id_type=MESH,
        )

    def partner(chunk, place):
        later = order(me, place, n)
        if not early:
            return later
        ends, mids = jnp.int32(0), jnp.int32(0)
        for i, (end, mid) in enumerate(zip((2, 3, 1, 4, 5, 6, 7), (6, 7, 1, 2, 3, 4, 5))):
            ends, mids = jnp.where(place == i, end, ends), jnp.where(place == i, mid, mids)
        return jnp.where(chunk == 0, flipped(me, jnp.where(middle, mids, ends), n), later)

    def step(i, carry):
        chunk, place = i // n, i % n
        own = place == n - 1
        dest = jnp.where(own, me, partner(chunk, place))

        @pl.when(place == 0)
        def _():
            loading(chunk).wait()

        @pl.when((chunk == 0) & (dest == 0) & (band > 0))
        def _():
            halo(0, band - 1).wait_recv()

        @pl.when((chunk == 0) & (dest == n - 1) & (band < bands - 1))
        def _():
            halo(1, band + 1).wait_recv()

        rows = rows_of(chunk)
        position = lane + shift_rows[rows, :]
        index = position & (LANES - 1)
        below, above = position < 0, position >= LANES

        def turned(tile):
            columns = pl.ds(pl.multiple_of(dest * width + tile * LANES, LANES), LANES)
            return jnp.take_along_axis(wide[rows, columns], index, axis=1, mode="promise_in_bounds")

        side = jnp.where(own, 1, 0)
        before, here = turned(0), turned(1)
        for tile in range(tiles):
            after = turned(tile + 2)
            blocks[side, dest, rows, tile * LANES:(tile + 1) * LANES] = jnp.where(
                below, before, jnp.where(above, after, here)
            )
            before, here = here, after

        if early:
            @pl.when((chunk == 0) & (place == 4))
            def _():
                hear_side()

            @pl.when((chunk == 0) & (place == jnp.where(middle, 6, 4)))
            def _():
                hear_all()

        @pl.when(place > 0)
        def _():
            sending(chunk, partner(chunk, place - 1)).start()

        return carry

    lax.fori_loop(0, chunks * n, step, 0)

    lowest = -jnp.inf
    if by_pairs:
        pair = lax.broadcasted_iota(jnp.int32, (n * n, LANES), 0)

        def mark(w, held):
            return jnp.where(pair == starts[w] * n + lengths[w] - 1, 0.0, held)

        table[...] = lax.fori_loop(0, windows, mark, jnp.full((n * n, LANES), lowest, jnp.float32))

    group = 2 * LANES if width % (2 * LANES) == 0 else LANES

    def arrive(chunk):
        def one(source, carry):
            @pl.when(source != me)
            def _():
                receiving(chunk, source).wait_recv()
            return carry
        lax.fori_loop(0, n, one, 0)

    def search_pairs(chunk):
        rows = rows_of(chunk)

        def search(j, carry):
            columns = pl.ds(pl.multiple_of(j * group, group), group)
            prefix = [None]
            for source in range(n):
                value = blocks[1, source, rows, columns]
                prefix.append(value if source == 0 else prefix[-1] + value)
            best = None
            for length in range(1, n + 1):
                most = None
                for start in range(n + 1 - length):
                    total = prefix[length] if start == 0 else prefix[start + length] - prefix[start]
                    at = start * n + length - 1
                    mask = jnp.concatenate([table[at:at + 1, :]] * (group // LANES), axis=1)
                    total = total + mask
                    most = total if most is None else jnp.maximum(most, total)
                root = math.sqrt(8.0 * length)
                score = most * (1.0 / root) - 4.0 * length / root
                best = score if best is None else jnp.maximum(best, score)
            out[rows, columns] = best
            return carry

        lax.fori_loop(0, width // group, search, 0)

    def search_windows(chunk):
        rows = rows_of(chunk)
        table[0] = jnp.zeros((ROWS, width), jnp.float32)

        def add(source, total):
            total = total + blocks[1, source, rows, :]
            table[source + 1] = total
            return total

        lax.fori_loop(0, n, add, jnp.zeros((ROWS, width), jnp.float32))

        def search(w, best):
            total = table[starts[w] + lengths[w]] - table[starts[w]]
            weight = jnp.full((ROWS, width), lengths[w], jnp.int32).astype(jnp.float32)
            return jnp.maximum(best, (total - 4.0 * weight) / jnp.sqrt(8.0 * weight))

        out[rows, :] = lax.fori_loop(0, windows, search, jnp.full((ROWS, width), lowest, jnp.float32))

    def finish(chunk, carry):
        arrive(chunk)
        (search_pairs if by_pairs else search_windows)(chunk)
        return carry

    lax.fori_loop(0, chunks, finish, 0)

    def drain(i, carry):
        chunk, peer = i // n, i % n

        @pl.when(peer != me)
        def _():
            sending(chunk, peer).wait_send()
        return carry

    lax.fori_loop(0, chunks * n, drain, 0)

    @pl.when(band < bands - 1)
    def _():
        halo(0, band + 1).wait_send()

    @pl.when(band > 0)
    def _():
        halo(1, band - 1).wait_send()


def solution(mesh):
    n, bands = mesh.shape["seg"], mesh.shape["bins"]

    def on_device(segment_maps, bin_shifts, window_start, window_length):
        _, spins, bins = segment_maps.shape
        width = bins // n
        chunks = spins // ROWS
        by_pairs = n * (n + 1) // 2 <= window_start.shape[0]
        table = (n * n, LANES) if by_pairs else (n + 1, ROWS, width)
        return pl.pallas_call(
            functools.partial(kernel, n, bands, by_pairs),
            out_shape=pltpu.VMEM((spins, width), jnp.float32),
            in_specs=[pl.BlockSpec(memory_space=pl.ANY)] * 4,
            out_specs=pl.BlockSpec(memory_space=pltpu.VMEM),
            scratch_shapes=[
                pltpu.VMEM((spins, bins + 2 * LANES), jnp.float32),
                pltpu.VMEM((2, n, spins, width), jnp.float32),
                pltpu.VMEM((spins, LANES), jnp.int32),
                pltpu.VMEM(table, jnp.float32),
                pltpu.SMEM(bin_shifts.shape, jnp.int32),
                pltpu.SMEM(window_start.shape, jnp.int32),
                pltpu.SMEM(window_length.shape, jnp.int32),
                pltpu.SemaphoreType.REGULAR,
                pltpu.SemaphoreType.REGULAR,
                pltpu.SemaphoreType.DMA((3,)),
                pltpu.SemaphoreType.DMA((chunks,)),
                pltpu.SemaphoreType.DMA((chunks, n)),
                pltpu.SemaphoreType.DMA((chunks, n)),
                pltpu.SemaphoreType.DMA((2,)),
                pltpu.SemaphoreType.DMA((2,)),
            ],
            compiler_params=pltpu.CompilerParams(collective_id=0, has_side_effects=True),
        )(segment_maps, bin_shifts, window_start, window_length)

    return jax.shard_map(
        on_device,
        mesh=mesh,
        in_specs=(P("seg", None, "bins"), P("seg", None), P(), P()),
        out_specs=P(None, ("bins", "seg")),
        check_vma=False,
    )
```

```python
import functools
import math

import jax
import jax.numpy as jnp
from jax import lax
from jax.experimental import pallas as pl
from jax.experimental.pallas import tpu as pltpu
from jax.sharding import PartitionSpec as P

MESH = pl.DeviceIdType.MESH
LANES = 128
ROWS = 8


def order(me, place, n):
    stride = n // 2
    first, partner = 0, place + stride
    while stride > 1:
        first += stride
        stride //= 2
        partner = jnp.where(place >= first, place - first + stride, partner)
    return flipped(me, partner, n)


def flipped(me, mask, n):
    other, bit = 0, 1
    while bit < n:
        other = other + (me // bit + mask // bit) % 2 * bit
        bit *= 2
    return other


def twin(me):
    return me + 1 - 2 * (me % 2)


def kernel(n, bands, by_pairs, maps, shifts_in, starts_in, lengths_in, out, wide, blocks, shift_rows, table,
           shifts, starts, lengths, side_in, all_in, small_sem, in_sem, send_sem, recv_sem, halo_send, halo_recv):
    me, band = lax.axis_index("seg"), lax.axis_index("bins")
    spins, bins = maps.shape[1], maps.shape[2]
    width = out.shape[1]
    tiles = width // LANES
    chunks = spins // ROWS
    windows = starts.shape[0]

    def rows_of(chunk):
        return pl.ds(pl.multiple_of(chunk * ROWS, ROWS), ROWS)

    def loading(chunk):
        return pltpu.make_async_copy(
            maps.at[0, rows_of(chunk), :], wide.at[rows_of(chunk), pl.ds(LANES, bins)], in_sem.at[chunk]
        )

    barrier = pltpu.get_barrier_semaphore()

    def greet(peer):
        pl.semaphore_signal(barrier, inc=1, device_id={"seg": peer}, device_id_type=MESH)

    early = n // 2 == 4
    pairs, pair_at = n // 2, me // 2
    low = pair_at < pairs // 2
    inner, outer = jnp.where(low, me + 2, me - 2), jnp.where(low, me - 2, me + 2)
    middle = jnp.where(low, pair_at == pairs // 2 - 1, pair_at == pairs // 2)
    has_outer = jnp.where(low, pair_at > 0, pair_at < pairs - 1)

    greet(twin(me))

    @pl.when(middle)
    def _():
        greet(inner)
        greet(twin(inner))

    @pl.when(has_outer)
    def _():
        greet(outer)
        greet(twin(outer))

    @pl.when(band > 0)
    def _():
        pl.semaphore_signal(barrier, inc=1, device_id={"bins": band - 1}, device_id_type=MESH)

    @pl.when(band < bands - 1)
    def _():
        pl.semaphore_signal(barrier, inc=1, device_id={"bins": band + 1}, device_id_type=MESH)

    small = [
        pltpu.make_async_copy(here, there, small_sem.at[i])
        for i, (here, there) in enumerate(((shifts_in, shifts), (starts_in, starts), (lengths_in, lengths)))
    ]
    for copy in small:
        copy.start()
    for chunk in range(chunks):
        loading(chunk).start()

    @pl.when(band == 0)
    def _():
        wide[:, :LANES] = jnp.zeros((spins, LANES), jnp.float32)

    @pl.when(band == bands - 1)
    def _():
        wide[:, bins + LANES:] = jnp.zeros((spins, LANES), jnp.float32)

    for copy in small:
        copy.wait()

    sublane = lax.broadcasted_iota(jnp.int32, (ROWS, LANES), 0)
    lane = lax.broadcasted_iota(jnp.int32, (ROWS, LANES), 1)
    for chunk in range(chunks):
        amounts = jnp.zeros((ROWS, LANES), jnp.int32)
        for row in range(ROWS):
            amounts = jnp.where(sublane == row, shifts[0, chunk * ROWS + row], amounts)
        shift_rows[chunk * ROWS:(chunk + 1) * ROWS, :] = amounts

    def partner(chunk, place):
        later = order(me, place, n)
        if not early:
            return later
        ends, mids = jnp.int32(0), jnp.int32(0)
        for i, (end, mid) in enumerate(zip((2, 3, 1, 4, 5, 6, 7), (6, 7, 1, 2, 3, 4, 5))):
            ends, mids = jnp.where(place == i, end, ends), jnp.where(place == i, mid, mids)
        return jnp.where(chunk == 0, flipped(me, jnp.where(middle, mids, ends), n), later)

    def align(chunk, dest, own):
        rows = rows_of(chunk)
        position = lane + shift_rows[rows, :]
        index = position & (LANES - 1)
        below, above = position < 0, position >= LANES

        def turned(tile):
            columns = pl.ds(pl.multiple_of(dest * width + tile * LANES, LANES), LANES)
            return jnp.take_along_axis(wide[rows, columns], index, axis=1, mode="promise_in_bounds")

        side = jnp.where(own, 1, 0)
        before, here = turned(0), turned(1)
        for tile in range(tiles):
            after = turned(tile + 2)
            blocks[side, dest, rows, tile * LANES:(tile + 1) * LANES] = jnp.where(
                below, before, jnp.where(above, after, here)
            )
            before, here = here, after

    if early:
        loading(0).wait()
        align(0, partner(0, 0), False)

    neighbours = jnp.where(band > 0, 1, 0) + jnp.where(band < bands - 1, 1, 0)
    pl.semaphore_wait(barrier, 3 + neighbours)

    def tell(sem, peer):
        pl.semaphore_signal(sem, inc=1, device_id={"seg": peer}, device_id_type=MESH)

    @pl.when(jnp.logical_not(has_outer))
    def _():
        tell(side_in, inner)

    def hear_side():
        @pl.when(has_outer)
        def _():
            pl.semaphore_wait(side_in, 1)

        @pl.when(has_outer & middle)
        def _():
            tell(all_in, inner)

        @pl.when(has_outer & jnp.logical_not(middle))
        def _():
            tell(side_in, inner)

    def hear_all():
        pl.semaphore_wait(all_in, 1)

        @pl.when(has_outer)
        def _():
            tell(all_in, outer)

    if not early:
        hear_side()
        hear_all()

    def halo(side, peer):
        source = bins - LANES if side == 0 else 0
        target = 0 if side == 0 else bins + LANES
        return pltpu.make_async_remote_copy(
            src_ref=maps.at[0, :, pl.ds(source, LANES)],
            dst_ref=wide.at[:, pl.ds(target, LANES)],
            send_sem=halo_send.at[side],
            recv_sem=halo_recv.at[side],
            device_id={"bins": peer},
            device_id_type=MESH,
        )

    @pl.when(band < bands - 1)
    def _():
        halo(0, band + 1).start()

    @pl.when(band > 0)
    def _():
        halo(1, band - 1).start()

    def sending(chunk, peer):
        return pltpu.make_async_remote_copy(
            src_ref=blocks.at[0, peer, rows_of(chunk), :],
            dst_ref=blocks.at[1, me, rows_of(chunk), :],
            send_sem=send_sem.at[chunk, peer],
            recv_sem=recv_sem.at[chunk, me],
            device_id={"seg": peer},
            device_id_type=MESH,
        )

    def receiving(chunk, source):
        return pltpu.make_async_remote_copy(
            src_ref=blocks.at[0, source, rows_of(chunk), :],
            dst_ref=blocks.at[1, source, rows_of(chunk), :],
            send_sem=send_sem.at[chunk, source],
            recv_sem=recv_sem.at[chunk, source],
            device_id={"seg": source},
            device_id_type=MESH,
        )

    def step(i, carry):
        chunk, place = i // n, i % n
        own = place == n - 1
        dest = jnp.where(own, me, partner(chunk, place))

        @pl.when((place == 0) & ((chunk > 0) | (not early)))
        def _():
            loading(chunk).wait()

        @pl.when((chunk == 0) & (dest == 0) & (band > 0))
        def _():
            halo(0, band - 1).wait_recv()

        @pl.when((chunk == 0) & (dest == n - 1) & (band < bands - 1))
        def _():
            halo(1, band + 1).wait_recv()

        @pl.when(i > 0 if early else i >= 0)
        def _():
            align(chunk, dest, own)

        if early:
            @pl.when((chunk == 0) & (place == 4))
            def _():
                hear_side()

            @pl.when((chunk == 0) & (place == jnp.where(middle, 6, 4)))
            def _():
                hear_all()

        @pl.when(place > 0)
        def _():
            sending(chunk, partner(chunk, place - 1)).start()

        return carry

    lax.fori_loop(0, chunks * n, step, 0)

    lowest = -jnp.inf
    if by_pairs:
        pair = lax.broadcasted_iota(jnp.int32, (n * n, LANES), 0)

        def mark(w, held):
            return jnp.where(pair == starts[w] * n + lengths[w] - 1, 0.0, held)

        table[...] = lax.fori_loop(0, windows, mark, jnp.full((n * n, LANES), lowest, jnp.float32))

    group = 2 * LANES if width % (2 * LANES) == 0 else LANES

    def arrive(chunk):
        def one(source, carry):
            @pl.when(source != me)
            def _():
                receiving(chunk, source).wait_recv()
            return carry
        lax.fori_loop(0, n, one, 0)

    def search_pairs(chunk):
        rows = rows_of(chunk)

        def search(j, carry):
            columns = pl.ds(pl.multiple_of(j * group, group), group)
            prefix = [None]
            for source in range(n):
                value = blocks[1, source, rows, columns]
                prefix.append(value if source == 0 else prefix[-1] + value)
            best = None
            for length in range(1, n + 1):
                most = None
                for start in range(n + 1 - length):
                    total = prefix[length] if start == 0 else prefix[start + length] - prefix[start]
                    at = start * n + length - 1
                    mask = jnp.concatenate([table[at:at + 1, :]] * (group // LANES), axis=1)
                    total = total + mask
                    most = total if most is None else jnp.maximum(most, total)
                root = math.sqrt(8.0 * length)
                score = most * (1.0 / root) - 4.0 * length / root
                best = score if best is None else jnp.maximum(best, score)
            out[rows, columns] = best
            return carry

        lax.fori_loop(0, width // group, search, 0, unroll=4 if width // group % 4 == 0 else 1)

    def search_windows(chunk):
        rows = rows_of(chunk)
        table[0] = jnp.zeros((ROWS, width), jnp.float32)

        def add(source, total):
            total = total + blocks[1, source, rows, :]
            table[source + 1] = total
            return total

        lax.fori_loop(0, n, add, jnp.zeros((ROWS, width), jnp.float32))

        def search(w, best):
            total = table[starts[w] + lengths[w]] - table[starts[w]]
            weight = jnp.full((ROWS, width), lengths[w], jnp.int32).astype(jnp.float32)
            return jnp.maximum(best, (total - 4.0 * weight) / jnp.sqrt(8.0 * weight))

        out[rows, :] = lax.fori_loop(0, windows, search, jnp.full((ROWS, width), lowest, jnp.float32))

    def finish(chunk, carry):
        arrive(chunk)
        (search_pairs if by_pairs else search_windows)(chunk)
        return carry

    lax.fori_loop(0, chunks, finish, 0)

    def drain(i, carry):
        chunk, peer = i // n, i % n

        @pl.when(peer != me)
        def _():
            sending(chunk, peer).wait_send()
        return carry

    lax.fori_loop(0, chunks * n, drain, 0)

    @pl.when(band < bands - 1)
    def _():
        halo(0, band + 1).wait_send()

    @pl.when(band > 0)
    def _():
        halo(1, band - 1).wait_send()


def solution(mesh):
    n, bands = mesh.shape["seg"], mesh.shape["bins"]

    def on_device(segment_maps, bin_shifts, window_start, window_length):
        _, spins, bins = segment_maps.shape
        width = bins // n
        chunks = spins // ROWS
        by_pairs = n * (n + 1) // 2 <= window_start.shape[0]
        table = (n * n, LANES) if by_pairs else (n + 1, ROWS, width)
        return pl.pallas_call(
            functools.partial(kernel, n, bands, by_pairs),
            out_shape=pltpu.VMEM((spins, width), jnp.float32),
            in_specs=[pl.BlockSpec(memory_space=pl.ANY)] * 4,
            out_specs=pl.BlockSpec(memory_space=pltpu.VMEM),
            scratch_shapes=[
                pltpu.VMEM((spins, bins + 2 * LANES), jnp.float32),
                pltpu.VMEM((2, n, spins, width), jnp.float32),
                pltpu.VMEM((spins, LANES), jnp.int32),
                pltpu.VMEM(table, jnp.float32),
                pltpu.SMEM(bin_shifts.shape, jnp.int32),
                pltpu.SMEM(window_start.shape, jnp.int32),
                pltpu.SMEM(window_length.shape, jnp.int32),
                pltpu.SemaphoreType.REGULAR,
                pltpu.SemaphoreType.REGULAR,
                pltpu.SemaphoreType.DMA((3,)),
                pltpu.SemaphoreType.DMA((chunks,)),
                pltpu.SemaphoreType.DMA((chunks, n)),
                pltpu.SemaphoreType.DMA((chunks, n)),
                pltpu.SemaphoreType.DMA((2,)),
                pltpu.SemaphoreType.DMA((2,)),
            ],
            compiler_params=pltpu.CompilerParams(collective_id=0, has_side_effects=True),
        )(segment_maps, bin_shifts, window_start, window_length)

    return jax.shard_map(
        on_device,
        mesh=mesh,
        in_specs=(P("seg", None, "bins"), P("seg", None), P(), P()),
        out_specs=P(None, ("bins", "seg")),
        check_vma=False,
    )
```
